512 devices in a mesh: cp: 128 (over z, y, core), tp: 4 (over x).
Axes of the slice: x: 4, y: 8, z: 8, core: 2. Of those that a mesh axis runs over, the one named last changes fastest.
Arguments:
- queries: bfloat16 [49152, 4096], P('cp', 'tp'), may hold values from -56 to 56
- keys: bfloat16 [49152, 1024], P('cp', 'tp'), may hold values from -6 to 6
- values: bfloat16 [49152, 1024], P('cp', 'tp'), may hold values from -6 to 6
- lengths: int32 [32], replicated, may hold values from 1 to 2689, 49152 in all
Outputs:
- attended: bfloat16 [49152, 4096], P('cp', 'tp')
The draws below stay inside these ranges and needn't reach their ends.
Inputs may be any that keep to these rules, and one draw needn't show every extreme that they name: `lengths`: the 32 documents fill the 49152 tokens; each has at most 2689 tokens and one has exactly 2689.
All inputs are finite; a program needn't handle non-finite values.
Results may differ from the reference program's by a relative error of at most 0.0065.
Values may be sent and summed in bfloat16 or wider, within the bound.
No kernel may reach another device: no remote copies, remote signals or barrier semaphores. Data moves between devices by JAX's collectives and lax.ppermute only.
A program may use at most 64 MiB of HBM per device.

```python
import math
import jax
import jax.numpy as jnp
import numpy as np
from jax import lax

HEADS = 32
KV_HEADS = 8
HEAD_DIM = 128
TOK_DEV = 384
SPAN = 8
DOC_MOST = 2689
NDOCS = 32
TOKENS = 49152
N_CP = 128


def shared_keys(key):
    base = jnp.clip(jax.random.normal(jax.random.fold_in(key, 11), (TOKENS, KV_HEADS * HEAD_DIM), jnp.float32), -4.5, 4.5)
    return base


def draw_keys(key, part):
    return shared_keys(key).astype(jnp.bfloat16)


def draw_queries(key, part):
    base = jnp.clip(jax.random.normal(jax.random.fold_in(key, 13), (TOKENS, HEADS * HEAD_DIM), jnp.float32), -4.5, 4.5)
    return base.astype(jnp.bfloat16)


def levels(own_key, shape, pieces, least, largest):
    def one(dim, parts):
        draws = jax.random.uniform(jax.random.fold_in(jax.random.fold_in(own_key, 6), dim), (parts,), jnp.float32, least / len(pieces), largest / len(pieces))
        return jnp.repeat(jnp.exp(draws), shape[dim] // parts).reshape((-1,) + (1,) * (len(shape) - dim - 1))

    factor_of = one(*pieces[0])
    for cut in pieces[1:]:
        factor_of = factor_of * one(*cut)
    return factor_of


def split_up(count, total, most, slope):
    loads = [(1 << 20) // math.isqrt(standing ** slope) + 1 for standing in range(2, count + 1)]
    spare, counts = total - most - (count - 1), [1] * (count - 1)
    while spare > 0:
        free = [i for i in range(count - 1) if counts[i] < most]
        whole, left = sum([loads[i] for i in free]), spare
        for i in free:
            addition = min(most - counts[i], max(1, left * loads[i] // whole), spare)
            counts[i] = counts[i] + addition
            spare = spare - addition
    return np.array([most] + counts)


def ragged_sizes(stream_key, amount, total, reach, slope):
    if amount == 2:
        one = jax.random.randint(stream_key, (), max(1, total - reach), min(reach, total - 1) + 1)
        return jnp.stack([one, total - one])
    sizes = jnp.asarray(split_up(amount, total, reach, slope), jnp.int32)
    couples = (amount - 1) // 2
    giver, receiver = sizes[1:1 + 2 * couples:2], sizes[2:2 + 2 * couples:2]
    margin = jnp.minimum(giver - 1, reach - receiver)
    shifted = jax.random.randint(jax.random.fold_in(stream_key, 1), (couples,), 0, 1 << 20) % (margin + 1)
    sizes = sizes.at[1:1 + 2 * couples:2].set(giver - shifted).at[2:2 + 2 * couples:2].set(receiver + shifted)
    return sizes[jax.random.permutation(jax.random.fold_in(stream_key, 2), amount)]


def scatter_about(key, extent, deviation, reach, split=(), kind=jnp.bfloat16):
    drawn = deviation * jax.random.normal(key, extent, jnp.float32)
    if split:
        drawn = drawn * levels(key, extent, split, -0.22, 0.18)
    return jnp.clip(drawn, -reach, reach).astype(kind)


def setup_inputs(seed: int = 0) -> dict:
    key_of = jax.random.split(jax.random.key(seed), 5)
    return {
        "queries": draw_queries(jax.random.fold_in(key_of[4], 71), 0),
        "keys": draw_keys(jax.random.fold_in(key_of[4], 71), 0),
        "values": scatter_about(key_of[2], (TOKENS, KV_HEADS * HEAD_DIM), 1.0, 6.0, ((0, 128), (1, 4))),
        "lengths": ragged_sizes(key_of[3], NDOCS, TOKENS, DOC_MOST, 2).astype(jnp.int32),
    }


def document_of(doc_starts, position):
    return jnp.sum((doc_starts[None, :] <= position[:, None]).astype(jnp.int32), axis=1) - 1


def reference(queries, keys, values, lengths):
    doc_ends = jnp.cumsum(lengths)
    doc_starts = doc_ends - lengths
    group_size = HEADS // KV_HEADS
    padding = (SPAN - 1) * TOK_DEV
    window = SPAN * TOK_DEV
    logit_scale_factor = HEAD_DIM ** -0.5
    key_pad = jnp.concatenate([jnp.zeros((padding, keys.shape[1]), keys.dtype), keys], axis=0)
    value_pad = jnp.concatenate([jnp.zeros((padding, values.shape[1]), values.dtype), values], axis=0)

    def one_block(block_index):
        anchor = (block_index * TOK_DEV).astype(jnp.int32)
        query_matrix_rows = lax.dynamic_slice_in_dim(queries, anchor, TOK_DEV, 0).astype(jnp.float32)
        query_matrix_rows = query_matrix_rows.reshape(TOK_DEV, KV_HEADS, group_size, HEAD_DIM)
        key_matrix_rows = lax.dynamic_slice_in_dim(key_pad, anchor, window, 0).astype(jnp.float32)
        key_matrix_rows = key_matrix_rows.reshape(window, KV_HEADS, HEAD_DIM)
        value_matrix_rows = lax.dynamic_slice_in_dim(value_pad, anchor, window, 0).astype(jnp.float32)
        value_matrix_rows = value_matrix_rows.reshape(window, KV_HEADS, HEAD_DIM)
        query_pos = anchor + jnp.arange(TOK_DEV, dtype=jnp.int32)
        key_pos = anchor - padding + jnp.arange(window, dtype=jnp.int32)
        allowed = (document_of(doc_starts, query_pos)[:, None] == document_of(doc_starts, key_pos)[None, :])
        allowed = allowed & (key_pos[None, :] <= query_pos[:, None]) & (key_pos[None, :] >= 0)
        attention_logits = jnp.einsum("yxau,kxu->xayk", query_matrix_rows, key_matrix_rows) * logit_scale_factor
        attention_logits = jnp.where(allowed, attention_logits, -1e30)
        row_max = jnp.max(attention_logits, axis=-1)
        weights = jnp.where(allowed, jnp.exp(attention_logits - row_max[..., None]), 0.0)
        total = jnp.sum(weights, axis=-1)
        lower_bound = weights.astype(jnp.bfloat16).astype(jnp.float32)
        weighted_value_sum = jnp.einsum("cqla,acf->cqlf", lower_bound, value_matrix_rows)
        result = weighted_value_sum / total[..., None]
        return result.transpose(2, 0, 1, 3).reshape(TOK_DEV, HEADS * HEAD_DIM).astype(jnp.bfloat16)

    blocks = lax.map(one_block, jnp.arange(N_CP, dtype=jnp.int32))
    return blocks.reshape(TOKENS, HEADS * HEAD_DIM)
```

```python
import functools

import jax
import jax.numpy as jnp
from jax import lax
from jax.experimental import pallas as pl
from jax.experimental.pallas import tpu as pltpu
from jax.sharding import PartitionSpec as P

HEAD_DIM = 128
RING = 8
TILE = 256
LANES = 128
NEG = -1e30
SCALE = HEAD_DIM**-0.5 * 1.4426950408889634
NONE = 1 << 20


def shifted(pairs):
    return [(a, b) for a, b in pairs if b is not None]


def routes(count):
    chips = count // 2
    dev = lambda n, c: 2 * n + c
    back = lambda n: n - n % RING + (n % RING - RING // 4) % RING
    inside = [n for n in range(chips) if n + 3 < chips]
    return {
        "cross": [(dev(n, c), dev(n + 1, 1 - c)) for n in range(chips - 1) for c in (0, 1)],
        "ahead": [(dev(n, c), dev(n + 1, c)) for n in range(chips - 1) for c in (0, 1)],
        "swap": [(dev(n, c), dev(n, 1 - c)) for n in range(chips) for c in (0, 1)],
        "mate": [(dev(n, 0), dev(n, 1)) for n in range(chips)],
        "back1": [(dev(n, 1), dev(back(n), 0)) for n in inside],
        "back2": [(dev(back(n), 0), dev((n + 4) % chips, 0)) for n in inside],
        "last": [(dev((n + 4) % chips, 0), dev(n + 3, 0)) for n in inside]
        + [(dev(n, 1), dev(n + 1, 1)) for n in range(chips - 1)],
    }


def attend_kernel(blocks, first, final, tok, heads, group, *refs):
    refs = list(refs)
    lengths, q_ref = refs.pop(0), refs.pop(0)
    kv_refs = [refs.pop(0) for _ in blocks]
    state_in = None if first else refs.pop(0)
    out_ref = refs.pop(0)
    state = refs.pop(0) if final else out_ref
    me = lax.axis_index("cp")
    anchor = me * tok
    odd = me % 2 == 1
    rows = group * tok
    tiles = rows // TILE
    chunks = tok // LANES

    lane = lax.broadcasted_iota(jnp.int32, (1, LANES), 1)
    pos = [anchor + k * LANES + lane for k in range(chunks)]
    low = [jnp.zeros((1, LANES), jnp.int32) for _ in range(chunks)]
    begin = jnp.int32(0)
    lead = jnp.int32(0)
    for d in range(lengths.shape[0]):
        low = [jnp.where(p >= begin, begin, l) for p, l in zip(pos, low)]
        lead = jnp.where(begin <= anchor, begin, lead)
        begin = begin + lengths[d]

    def wide(parts, t):
        per = TILE // LANES
        return jnp.concatenate([parts[(t * per + k) % chunks] for k in range(per)], axis=1)

    def query_tile(g, t):
        at, left, parts = t * TILE, TILE, []
        while left:
            r, row = divmod(at, tok)
            n = min(left, tok - row)
            h = g * group + r
            parts.append(q_ref[row : row + n, h * HEAD_DIM : (h + 1) * HEAD_DIM])
            at, left = at + n, left - n
        return parts[0] if len(parts) == 1 else jnp.concatenate(parts, axis=0)

    def fold(kv_ref, start, diagonal, fresh, source):
        key_row = start + lax.broadcasted_iota(jnp.int32, (tok, TILE), 0)
        for g in range(heads):
            key = kv_ref[0, :, g * HEAD_DIM : (g + 1) * HEAD_DIM]
            value = kv_ref[1, :, g * HEAD_DIM : (g + 1) * HEAD_DIM]
            for t in range(tiles):
                n = g * tiles + t
                score = lax.dot_general(
                    key, query_tile(g, t), (((1,), (1,)), ((), ())), preferred_element_type=jnp.float32
                )
                live = key_row >= wide(low, t)
                if diagonal:
                    live = live & (key_row <= wide(pos, t))
                score = jnp.where(live, score, NEG)
                top = jnp.max(score, axis=0, keepdims=True)
                if not fresh:
                    old = source[n, HEAD_DIM : HEAD_DIM + 1, :]
                    top = jnp.maximum(top, old)
                weight = jnp.exp2((score - top) * SCALE)
                total = jnp.sum(weight, axis=0, keepdims=True)
                acc = lax.dot_general(
                    value, weight.astype(jnp.bfloat16), (((0,), (0,)), ((), ())), preferred_element_type=jnp.float32
                )
                if not fresh:
                    fade = jnp.exp2((old - top) * SCALE)
                    total = total + source[n, HEAD_DIM + 1 : HEAD_DIM + 2, :] * fade
                    acc = acc + source[n, :HEAD_DIM, :] * fade
                state[n, :HEAD_DIM, :] = acc
                state[n, HEAD_DIM : HEAD_DIM + 1, :] = top
                state[n, HEAD_DIM + 1 : HEAD_DIM + 2, :] = total

    if not first and final:
        state[...] = state_in[...]
    for j, (kv_ref, (even_back, odd_back)) in enumerate(zip(kv_refs, blocks)):
        if first and j == 0:
            fold(kv_ref, anchor, True, True, None)
            continue
        start = anchor - jnp.where(odd, odd_back, even_back) * tok
        pl.when((start >= 0) & (lead < start + tok))(
            functools.partial(fold, kv_ref, start, False, False, state)
        )

    if final:
        for g in range(heads):
            for t in range(tiles):
                n = g * tiles + t
                share = 1.0 / state[n, HEAD_DIM + 1 : HEAD_DIM + 2, :]
                done = (state[n, :HEAD_DIM, :] * share).T.astype(jnp.bfloat16)
                at, left = t * TILE, TILE
                while left:
                    r, row = divmod(at, tok)
                    m = min(left, tok - row)
                    h = g * group + r
                    o = at - t * TILE
                    out_ref[row : row + m, h * HEAD_DIM : (h + 1) * HEAD_DIM] = done[o : o + m, :]
                    at, left = at + m, left - m


def attend(lengths, queries, kvs, blocks, state, final):
    tok, width = queries.shape
    heads = kvs[0].shape[2] // HEAD_DIM
    group = width // kvs[0].shape[2]
    count = heads * group * tok // TILE
    first = state is None
    state_shape = jax.ShapeDtypeStruct((count, HEAD_DIM + 8, TILE), jnp.float32)
    vmem = pl.BlockSpec(memory_space=pltpu.VMEM)
    args = [lengths, queries, *kvs] + ([] if first else [state])
    aliases = {} if first or final else {len(args) - 1: 0}
    flops = 4 * tok * tok * width * len(kvs)
    return pl.pallas_call(
        functools.partial(attend_kernel, blocks, first, final, tok, heads, group),
        out_shape=jax.ShapeDtypeStruct((tok, width), jnp.bfloat16) if final else state_shape,
        in_specs=[pl.BlockSpec(memory_space=pltpu.SMEM)] + [vmem] * (len(args) - 1),
        out_specs=vmem,
        scratch_shapes=[pltpu.VMEM(state_shape.shape, jnp.float32)] if final else [],
        input_output_aliases=aliases,
        compiler_params=pltpu.CompilerParams(vmem_limit_bytes=24 << 20),
        cost_estimate=pl.CostEstimate(flops=flops, bytes_accessed=1 << 20, transcendentals=0),
    )(*args)


def body(queries, keys, values, lengths):
    ways = routes(lax.axis_size("cp"))
    move = lambda x, way: lax.ppermute(x, "cp", ways[way])
    after = lax.optimization_barrier
    step = functools.partial(attend, lengths, queries)
    even = lax.axis_index("cp") % 2 == 0
    own = jnp.stack([keys, values])
    got1 = move(own, "cross")
    far1 = move(own, "back1")
    mate0 = move(own, "mate")
    state = step([own], [(0, 0)], None, False)
    state, got1, far1, mate0 = after((state, got1, far1, mate0))
    got2 = move(got1, "ahead")
    far2 = move(far1, "back2")
    mate1 = move(got1, "swap")
    state = step([mate0, got1], [(NONE, 1), (1, 3)], state, False)
    state, mate1 = after((state, mate1))
    state = step([mate1], [(2, 2)], state, False)
    state, got2, far2 = after((state, got2, far2))
    got3 = move(jnp.where(even, far2, got2), "last")
    mate2 = move(got2, "swap")
    state = step([got2, far2], [(3, 5), (7, NONE)], state, False)
    state, mate2 = after((state, mate2))
    state = step([mate2], [(4, 4)], state, False)
    state, got3 = after((state, got3))
    mate3 = move(got3, "swap")
    state = step([got3], [(5, 7)], state, False)
    state, mate3 = after((state, mate3))
    return step([mate3], [(6, 6)], state, True)


def solution(mesh):
    in_specs = (P("cp", "tp"), P("cp", "tp"), P("cp", "tp"), P())
    out_specs = P("cp", "tp")
    return jax.shard_map(body, mesh=mesh, in_specs=in_specs, out_specs=out_specs, check_vma=False)
```

```python
import functools

import jax
import jax.numpy as jnp
from jax import lax
from jax.experimental import pallas as pl
from jax.experimental.pallas import tpu as pltpu
from jax.sharding import PartitionSpec as P

HEAD_DIM = 128
RING = 8
TILE = 512
LANES = 128
NEG = -1e30
SCALE = HEAD_DIM**-0.5 * 1.4426950408889634
NONE = 1 << 20
DEPTH = 2
BATCH = 1


def shifted(pairs):
    return [(a, b) for a, b in pairs if b is not None]


def routes(count):
    chips = count // 2
    dev = lambda n, c: 2 * n + c
    back = lambda n: n - n % RING + (n % RING - RING // 4) % RING
    inside = [n for n in range(chips) if n + 3 < chips]
    return {
        "cross": [(dev(n, c), dev(n + 1, 1 - c)) for n in range(chips - 1) for c in (0, 1)],
        "ahead": [(dev(n, c), dev(n + 1, c)) for n in range(chips - 1) for c in (0, 1)],
        "swap": [(dev(n, c), dev(n, 1 - c)) for n in range(chips) for c in (0, 1)],
        "mate": [(dev(n, 0), dev(n, 1)) for n in range(chips)],
        "back1": [(dev(n, 1), dev(back(n), 0)) for n in inside],
        "back2": [(dev(back(n), 0), dev((n + 4) % chips, 0)) for n in inside],
        "last": [(dev((n + 4) % chips, 0), dev(n + 3, 0)) for n in inside]
        + [(dev(n, 1), dev(n + 1, 1)) for n in range(chips - 1)],
    }


def attend_kernel(blocks, first, final, tok, heads, group, *refs):
    refs = list(refs)
    lengths, q_ref = refs.pop(0), refs.pop(0)
    kv_refs = [refs.pop(0) for _ in blocks]
    state_in = None if first else refs.pop(0)
    out_ref = refs.pop(0)
    s_ref, p_ref, mask_ref = refs.pop(0), refs.pop(0), refs.pop(0)
    state = refs.pop(0) if final else out_ref
    me = lax.axis_index("cp")
    anchor = me * tok
    odd = me % 2 == 1
    rows = group * tok
    tiles = rows // TILE
    chunks = tok // LANES

    lane = lax.broadcasted_iota(jnp.int32, (1, LANES), 1)
    pos = [anchor + k * LANES + lane for k in range(chunks)]
    low = [jnp.zeros((1, LANES), jnp.int32) for _ in range(chunks)]
    begin = jnp.int32(0)
    lead = jnp.int32(0)
    for d in range(lengths.shape[0]):
        low = [jnp.where(p >= begin, begin, l) for p, l in zip(pos, low)]
        lead = jnp.where(begin <= anchor, begin, lead)
        begin = begin + lengths[d]

    def wide(parts, t):
        per = TILE // LANES
        return jnp.concatenate([parts[(t * per + k) % chunks] for k in range(per)], axis=1)

    def query_tile(g, t):
        at, left, parts = t * TILE, TILE, []
        while left:
            r, row = divmod(at, tok)
            n = min(left, tok - row)
            h = g * group + r
            parts.append(q_ref[row : row + n, h * HEAD_DIM : (h + 1) * HEAD_DIM])
            at, left = at + n, left - n
        return parts[0] if len(parts) == 1 else jnp.concatenate(parts, axis=0)

    def fold(kv_ref, mode, source):
        fresh = mode == "own"
        total_tiles = heads * tiles
        tops, shifts, fades = {}, {}, {}

        def score_stage(n):
            g, t = divmod(n, tiles)
            key = kv_ref[0, :, g * HEAD_DIM : (g + 1) * HEAD_DIM]
            score = lax.dot_general(
                key, query_tile(g, t), (((1,), (1,)), ((), ())), preferred_element_type=jnp.float32
            )
            if mode == "own":
                score = score + wide([mask_ref[:, k * LANES : (k + 1) * LANES] for k in range(chunks)], t)
            elif mode == "part":
                score = score + wide([mask_ref[:, :LANES]] * chunks, t)
            s_ref[n % DEPTH] = score
            top = jnp.max(score, axis=0, keepdims=True)
            shifts[n] = top
            if not fresh:
                joins = wide(low, t) == lead
                old = source[n, HEAD_DIM : HEAD_DIM + 1, :]
                top = jnp.where(joins, jnp.maximum(top, old), old)
                shifts[n] = jnp.where(joins, top, -NEG)
                fades[n] = jnp.exp2((old - top) * SCALE)
            tops[n] = top

        def weight_stage(n):
            weight = jnp.exp2((s_ref[n % DEPTH] - shifts[n]) * SCALE)
            p_ref[n % DEPTH] = weight.astype(jnp.bfloat16)
            total = jnp.sum(weight, axis=0, keepdims=True)
            if not fresh:
                total = total + source[n, HEAD_DIM + 1 : HEAD_DIM + 2, :] * fades[n]
            state[n, HEAD_DIM : HEAD_DIM + 1, :] = tops[n]
            state[n, HEAD_DIM + 1 : HEAD_DIM + 2, :] = total

        def value_stage(n):
            g, t = divmod(n, tiles)
            value = kv_ref[1, :, g * HEAD_DIM : (g + 1) * HEAD_DIM]
            acc = lax.dot_general(
                value, p_ref[n % DEPTH], (((0,), (0,)), ((), ())), preferred_element_type=jnp.float32
            )
            if not fresh:
                acc = acc + source[n, :HEAD_DIM, :] * fades[n]
            state[n, :HEAD_DIM, :] = acc

        for i in range(0, total_tiles + 2 * BATCH, BATCH):
            for k in range(BATCH):
                n = i + k
                if n < total_tiles:
                    score_stage(n)
                if 0 <= n - BATCH < total_tiles:
                    weight_stage(n - BATCH)
                if 0 <= n - 2 * BATCH < total_tiles:
                    value_stage(n - 2 * BATCH)

    if not first and final:
        state[...] = state_in[...]
    for j, (kv_ref, (even_back, odd_back)) in enumerate(zip(kv_refs, blocks)):
        if first and j == 0:
            key_row = anchor + lax.broadcasted_iota(jnp.int32, (tok, LANES), 0)
            for k in range(chunks):
                live = (key_row >= low[k]) & (key_row <= pos[k])
                mask_ref[:, k * LANES : (k + 1) * LANES] = jnp.where(live, 0.0, NEG)
            fold(kv_ref, "own", None)
            continue
        start = anchor - jnp.where(odd, odd_back, even_back) * tok

        @pl.when((start >= 0) & (lead < start + tok))
        def _():
            key_row = start + lax.broadcasted_iota(jnp.int32, (tok, LANES), 0)
            mask_ref[:, :LANES] = jnp.where(key_row >= lead, 0.0, NEG)
            fold(kv_ref, "part", state)

    if final:
        for g in range(heads):
            for t in range(tiles):
                n = g * tiles + t
                share = 1.0 / state[n, HEAD_DIM + 1 : HEAD_DIM + 2, :]
                done = (state[n, :HEAD_DIM, :] * share).T.astype(jnp.bfloat16)
                at, left = t * TILE, TILE
                while left:
                    r, row = divmod(at, tok)
                    m = min(left, tok - row)
                    h = g * group + r
                    o = at - t * TILE
                    out_ref[row : row + m, h * HEAD_DIM : (h + 1) * HEAD_DIM] = done[o : o + m, :]
                    at, left = at + m, left - m


def small_call(kernel, outs, *args):
    vmem = pl.BlockSpec(memory_space=pltpu.VMEM)
    return pl.pallas_call(
        kernel,
        out_shape=outs,
        in_specs=[vmem] * len(args),
        out_specs=jax.tree.map(lambda _: vmem, outs),
        compiler_params=pltpu.CompilerParams(vmem_limit_bytes=4 << 20),
        cost_estimate=pl.CostEstimate(flops=1 << 20, bytes_accessed=1 << 20, transcendentals=0),
    )(*args)


def stack_kernel(k_ref, v_ref, out_ref):
    out_ref[0] = k_ref[...]
    out_ref[1] = v_ref[...]


def keep_kernel(q_ref, out_ref):
    out_ref[...] = q_ref[...]


def pick_kernel(even_ref, odd_ref, out_ref):
    odd = lax.axis_index("cp") % 2 == 1

    @pl.when(odd)
    def _():
        out_ref[...] = odd_ref[...]

    @pl.when(jnp.logical_not(odd))
    def _():
        out_ref[...] = even_ref[...]


def attend(lengths, queries, kvs, blocks, state, final):
    tok, width = queries.shape
    heads = kvs[0].shape[2] // HEAD_DIM
    group = width // kvs[0].shape[2]
    count = heads * group * tok // TILE
    first = state is None
    state_shape = jax.ShapeDtypeStruct((count, HEAD_DIM + 8, TILE), jnp.float32)
    vmem = pl.BlockSpec(memory_space=pltpu.VMEM)
    args = [lengths, queries, *kvs] + ([] if first else [state])
    aliases = {} if first or final else {len(args) - 1: 0}
    flops = 4 * tok * tok * width * len(kvs)
    return pl.pallas_call(
        functools.partial(attend_kernel, blocks, first, final, tok, heads, group),
        out_shape=jax.ShapeDtypeStruct((tok, width), jnp.bfloat16) if final else state_shape,
        in_specs=[pl.BlockSpec(memory_space=pltpu.SMEM)] + [vmem] * (len(args) - 1),
        out_specs=vmem,
        scratch_shapes=[
            pltpu.VMEM((DEPTH, tok, TILE), jnp.float32),
            pltpu.VMEM((DEPTH, tok, TILE), jnp.bfloat16),
            pltpu.VMEM((tok, tok), jnp.float32),
            *([pltpu.VMEM(state_shape.shape, jnp.float32)] if final else []),
        ],
        input_output_aliases=aliases,
        compiler_params=pltpu.CompilerParams(vmem_limit_bytes=16 << 20),
        cost_estimate=pl.CostEstimate(flops=flops, bytes_accessed=1 << 20, transcendentals=0),
    )(*args)


def body(queries, keys, values, lengths):
    ways = routes(lax.axis_size("cp"))
    move = lambda x, way: lax.ppermute(x, "cp", ways[way])
    after = lax.optimization_barrier
    step = functools.partial(attend, lengths, queries)
    own = small_call(stack_kernel, jax.ShapeDtypeStruct((2, *keys.shape), keys.dtype), keys, values)
    got1 = move(own, "cross")
    far1 = move(own, "back1")
    mate0 = move(own, "mate")
    state = step([own], [(0, 0)], None, False)
    state, got1, far1, mate0 = after((state, got1, far1, mate0))
    got2 = move(got1, "ahead")
    far2 = move(far1, "back2")
    mate1 = move(got1, "swap")
    state = step([mate0, got1], [(NONE, 1), (1, 3)], state, False)
    state, mate1 = after((state, mate1))
    state = step([mate1], [(2, 2)], state, False)
    state, got2, far2 = after((state, got2, far2))
    got3 = move(small_call(pick_kernel, jax.ShapeDtypeStruct(got2.shape, got2.dtype), far2, got2), "last")
    mate2 = move(got2, "swap")
    state = step([got2, far2], [(3, 5), (7, NONE)], state, False)
    state, mate2 = after((state, mate2))
    state = step([mate2], [(4, 4)], state, False)
    state, got3 = after((state, got3))
    mate3 = move(got3, "swap")
    state = step([got3], [(5, 7)], state, False)
    state, mate3 = after((state, mate3))
    return step([mate3], [(6, 6)], state, True)


def solution(mesh):
    in_specs = (P("cp", "tp"), P("cp", "tp"), P("cp", "tp"), P())
    out_specs = P("cp", "tp")
    return jax.shard_map(body, mesh=mesh, in_specs=in_specs, out_specs=out_specs, check_vma=False)
```

```python
import functools

import jax
import jax.numpy as jnp
from jax import lax
from jax.experimental import pallas as pl
from jax.experimental.pallas import tpu as pltpu
from jax.sharding import PartitionSpec as P


HEAD_DIM = 128
RING = 8
TILE = 512
LANES = 128
NEG = -1e30
SCALE = HEAD_DIM**-0.5 * 1.4426950408889634
NONE = 1 << 20
DEPTH = 2
BATCH = 1


def routes(count):
    chips = count // 2
    dev = lambda n, c: 2 * n + c
    back = lambda n: n - n % RING + (n % RING - RING // 4) % RING
    inside = [n for n in range(chips) if n + 3 < chips]
    return {
        "cross": [(dev(n, c), dev(n + 1, 1 - c)) for n in range(chips - 1) for c in (0, 1)],
        "ahead": [(dev(n, c), dev(n + 1, c)) for n in range(chips - 1) for c in (0, 1)],
        "swap": [(dev(n, c), dev(n, 1 - c)) for n in range(chips) for c in (0, 1)],
        "mate": [(dev(n, 0), dev(n, 1)) for n in range(chips)],
        "back1": [(dev(n, 1), dev(back(n), 0)) for n in inside],
        "back2": [(dev(back(n), 0), dev((n + 4) % chips, 0)) for n in inside],
        "last": [(dev((n + 4) % chips, 0), dev(n + 3, 0)) for n in inside]
        + [(dev(n, 1), dev(n + 1, 1)) for n in range(chips - 1)],
    }


def attend_kernel(blocks, first, final, tok, heads, group, *refs):
    refs = list(refs)
    lengths, q_ref = refs.pop(0), refs.pop(0)
    kv_refs = [refs.pop(0) for _ in blocks]
    state_in = None if first else refs.pop(0)
    out_ref = refs.pop(0)
    s_ref, p_ref, mask_ref = refs.pop(0), refs.pop(0), refs.pop(0)
    state = refs.pop(0) if final else out_ref
    me = lax.axis_index("cp")
    anchor = me * tok
    odd = me % 2 == 1
    rows = group * tok
    tiles = rows // TILE
    chunks = tok // LANES

    lane = lax.broadcasted_iota(jnp.int32, (1, LANES), 1)
    pos = [anchor + k * LANES + lane for k in range(chunks)]
    low = [jnp.zeros((1, LANES), jnp.int32) for _ in range(chunks)]
    begin = jnp.int32(0)
    lead = jnp.int32(0)
    for d in range(lengths.shape[0]):
        low = [jnp.where(p >= begin, begin, l) for p, l in zip(pos, low)]
        lead = jnp.where(begin <= anchor, begin, lead)
        begin = begin + lengths[d]

    def wide(parts, t):
        per = TILE // LANES
        return jnp.concatenate([parts[(t * per + k) % chunks] for k in range(per)], axis=1)

    def query_tile(g, t):
        at, left, parts = t * TILE, TILE, []
        while left:
            r, row = divmod(at, tok)
            n = min(left, tok - row)
            h = g * group + r
            parts.append(q_ref[row : row + n, h * HEAD_DIM : (h + 1) * HEAD_DIM])
            at, left = at + n, left - n
        return parts[0] if len(parts) == 1 else jnp.concatenate(parts, axis=0)

    def fold(kv_ref, mode, source):
        fresh = mode == "own"
        total_tiles = heads * tiles
        tops, shifts, fades = {}, {}, {}

        def score_stage(n):
            g, t = divmod(n, tiles)
            key = kv_ref[0, :, g * HEAD_DIM : (g + 1) * HEAD_DIM]
            score = lax.dot_general(
                key, query_tile(g, t), (((1,), (1,)), ((), ())), preferred_element_type=jnp.float32
            )
            if mode == "own":
                score = score + wide([mask_ref[:, k * LANES : (k + 1) * LANES] for k in range(chunks)], t)
            elif mode == "part":
                score = score + wide([mask_ref[:, :LANES]] * chunks, t)
            s_ref[n % DEPTH] = score
            top = jnp.max(score, axis=0, keepdims=True)
            shifts[n] = top
            if not fresh:
                joins = wide(low, t) == lead
                old = source[n, HEAD_DIM : HEAD_DIM + 1, :]
                top = jnp.where(joins, jnp.maximum(top, old), old)
                shifts[n] = jnp.where(joins, top, -NEG)
                fades[n] = jnp.exp2((old - top) * SCALE)
            tops[n] = top

        def weight_stage(n):
            weight = jnp.exp2((s_ref[n % DEPTH] - shifts[n]) * SCALE)
            p_ref[n % DEPTH] = weight.astype(jnp.bfloat16)
            total = jnp.sum(weight, axis=0, keepdims=True)
            if not fresh:
                total = total + source[n, HEAD_DIM + 1 : HEAD_DIM + 2, :] * fades[n]
            state[n, HEAD_DIM : HEAD_DIM + 1, :] = tops[n]
            state[n, HEAD_DIM + 1 : HEAD_DIM + 2, :] = total

        def value_stage(n):
            g, _ = divmod(n, tiles)
            value = kv_ref[1, :, g * HEAD_DIM : (g + 1) * HEAD_DIM]
            acc = lax.dot_general(
                value, p_ref[n % DEPTH], (((0,), (0,)), ((), ())), preferred_element_type=jnp.float32
            )
            if not fresh:
                acc = acc + source[n, :HEAD_DIM, :] * fades[n]
            state[n, :HEAD_DIM, :] = acc

        for i in range(0, total_tiles + 2 * BATCH, BATCH):
            for k in range(BATCH):
                n = i + k
                if n < total_tiles:
                    score_stage(n)
                if 0 <= n - BATCH < total_tiles:
                    weight_stage(n - BATCH)
                if 0 <= n - 2 * BATCH < total_tiles:
                    value_stage(n - 2 * BATCH)

    if not first and final:
        state[...] = state_in[...]
    for j, (kv_ref, (even_back, odd_back)) in enumerate(zip(kv_refs, blocks)):
        if first and j == 0:
            key_row = anchor + lax.broadcasted_iota(jnp.int32, (tok, LANES), 0)
            for k in range(chunks):
                live = (key_row >= low[k]) & (key_row <= pos[k])
                mask_ref[:, k * LANES : (k + 1) * LANES] = jnp.where(live, 0.0, NEG)
            fold(kv_ref, "own", None)
            continue
        start = anchor - jnp.where(odd, odd_back, even_back) * tok

        @pl.when((start >= 0) & (lead < start + tok))
        def _():
            key_row = start + lax.broadcasted_iota(jnp.int32, (tok, LANES), 0)
            mask_ref[:, :LANES] = jnp.where(key_row >= lead, 0.0, NEG)
            fold(kv_ref, "part", state)

    if final:
        for g in range(heads):
            for t in range(tiles):
                n = g * tiles + t
                share = 1.0 / state[n, HEAD_DIM + 1 : HEAD_DIM + 2, :]
                done = (state[n, :HEAD_DIM, :] * share).T.astype(jnp.bfloat16)
                at, left = t * TILE, TILE
                while left:
                    r, row = divmod(at, tok)
                    m = min(left, tok - row)
                    h = g * group + r
                    o = at - t * TILE
                    out_ref[row : row + m, h * HEAD_DIM : (h + 1) * HEAD_DIM] = done[o : o + m, :]
                    at, left = at + m, left - m


def small_call(kernel, outs, *args):
    vmem = pl.BlockSpec(memory_space=pltpu.VMEM)
    return pl.pallas_call(
        kernel,
        out_shape=outs,
        in_specs=[vmem] * len(args),
        out_specs=jax.tree.map(lambda _: vmem, outs),
        compiler_params=pltpu.CompilerParams(vmem_limit_bytes=4 << 20),
        cost_estimate=pl.CostEstimate(flops=1 << 20, bytes_accessed=1 << 20, transcendentals=0),
    )(*args)


def stack_kernel(k_ref, v_ref, out_ref):
    out_ref[0] = k_ref[...]
    out_ref[1] = v_ref[...]


def pick_kernel(even_ref, odd_ref, out_ref):
    odd = lax.axis_index("cp") % 2 == 1

    @pl.when(odd)
    def _():
        out_ref[...] = odd_ref[...]

    @pl.when(jnp.logical_not(odd))
    def _():
        out_ref[...] = even_ref[...]


def attend(lengths, queries, kvs, blocks, state, final):
    tok, width = queries.shape
    heads = kvs[0].shape[2] // HEAD_DIM
    group = width // kvs[0].shape[2]
    count = heads * group * tok // TILE
    first = state is None
    state_shape = jax.ShapeDtypeStruct((count, HEAD_DIM + 8, TILE), jnp.float32)
    vmem = pl.BlockSpec(memory_space=pltpu.VMEM)
    args = [lengths, queries, *kvs] + ([] if first else [state])
    aliases = {} if first or final else {len(args) - 1: 0}
    flops = 4 * tok * tok * width * len(kvs)
    return pl.pallas_call(
        functools.partial(attend_kernel, blocks, first, final, tok, heads, group),
        out_shape=jax.ShapeDtypeStruct((tok, width), jnp.bfloat16) if final else state_shape,
        in_specs=[pl.BlockSpec(memory_space=pltpu.SMEM)] + [vmem] * (len(args) - 1),
        out_specs=vmem,
        scratch_shapes=[
            pltpu.VMEM((DEPTH, tok, TILE), jnp.float32),
            pltpu.VMEM((DEPTH, tok, TILE), jnp.bfloat16),
            pltpu.VMEM((tok, tok), jnp.float32),
            *([pltpu.VMEM(state_shape.shape, jnp.float32)] if final else []),
        ],
        input_output_aliases=aliases,
        compiler_params=pltpu.CompilerParams(vmem_limit_bytes=16 << 20),
        cost_estimate=pl.CostEstimate(flops=flops, bytes_accessed=1 << 20, transcendentals=0),
    )(*args)


def body(queries, keys, values, lengths):
    ways = routes(lax.axis_size("cp"))

    def move(x, way):
        return lax.ppermute(x, "cp", ways[way])

    after = lax.optimization_barrier
    step = functools.partial(attend, lengths, queries)
    own = small_call(stack_kernel, jax.ShapeDtypeStruct((2, *keys.shape), keys.dtype), keys, values)
    got1 = move(own, "cross")
    far1 = move(own, "back1")
    mate0 = move(own, "mate")
    state = step([own], [(0, 0)], None, False)
    state, got1, mate0 = after((state, got1, mate0))
    got2 = move(got1, "ahead")
    far2 = move(far1, "back2")
    mate1 = move(got1, "swap")
    state = step([mate0, got1], [(NONE, 1), (1, 3)], state, False)
    state, mate1 = after((state, mate1))
    state = step([mate1], [(2, 2)], state, False)
    state, got2 = after((state, got2))
    got3 = move(small_call(pick_kernel, jax.ShapeDtypeStruct(got2.shape, got2.dtype), far2, got2), "last")
    mate2 = move(got2, "swap")
    state = step([got2, far2], [(3, 5), (7, NONE)], state, False)
    state, mate2 = after((state, mate2))
    state = step([mate2], [(4, 4)], state, False)
    state, got3 = after((state, got3))
    mate3 = move(got3, "swap")
    state = step([got3], [(5, 7)], state, False)
    state, mate3 = after((state, mate3))
    return step([mate3], [(6, 6)], state, True)


def solution(mesh):
    in_specs = (P("cp", "tp"), P("cp", "tp"), P("cp", "tp"), P())
    out_specs = P("cp", "tp")
    return jax.shard_map(body, mesh=mesh, in_specs=in_specs, out_specs=out_specs, check_vma=False)
```

```python
import functools

import jax
import jax.numpy as jnp
from jax import lax
from jax.experimental import pallas as pl
from jax.experimental.pallas import tpu as pltpu
from jax.sharding import PartitionSpec as P


HEAD_DIM = 128
RING = 8
TILE = 512
LANES = 128
NEG = -1e30
SCALE = HEAD_DIM**-0.5 * 1.4426950408889634
NONE = 1 << 20
DEPTH = 2
BATCH = 1


def routes(count):
    chips = count // 2
    dev = lambda n, c: 2 * n + c
    back = lambda n: n - n % RING + (n % RING - RING // 4) % RING
    inside = [n for n in range(chips) if n + 4 < chips]
    return {
        "cross": [(dev(n, c), dev(n + 1, 1 - c)) for n in range(chips - 1) for c in (0, 1)],
        "ahead": [(dev(n, c), dev(n + 1, c)) for n in range(chips - 1) for c in (0, 1)],
        "swap": [(dev(n, c), dev(n, 1 - c)) for n in range(chips) for c in (0, 1)],
        "back1": [(dev(n, 1), dev(back(n), 0)) for n in inside] + [(dev(n, 0), dev(n, 1)) for n in range(chips)],
        "back2": [(dev(back(n), 0), dev(n + 4, 0)) for n in inside],
    }


def attend_kernel(blocks, first, final, tok, heads, group, *refs):
    refs = list(refs)
    lengths, q_ref = refs.pop(0), refs.pop(0)
    kv_refs = []
    while len(kv_refs) < len(blocks):
        ref = refs.pop(0)
        kv_refs += [ref] if len(ref.shape) == 3 else [ref.at[j] for j in range(ref.shape[0])]
    state_in = None if first else refs.pop(0)
    out_ref = refs.pop(0)
    s_ref, p_ref, mask_ref = refs.pop(0), refs.pop(0), refs.pop(0)
    state = refs.pop(0) if final else out_ref
    me = lax.axis_index("cp")
    anchor = me * tok
    odd = me % 2 == 1
    rows = group * tok
    tiles = rows // TILE
    chunks = tok // LANES

    lane = lax.broadcasted_iota(jnp.int32, (1, LANES), 1)
    pos = [anchor + k * LANES + lane for k in range(chunks)]
    low = [jnp.zeros((1, LANES), jnp.int32) for _ in range(chunks)]
    begin = jnp.int32(0)
    lead = jnp.int32(0)
    for d in range(lengths.shape[0]):
        low = [jnp.where(p >= begin, begin, l) for p, l in zip(pos, low)]
        lead = jnp.where(begin <= anchor, begin, lead)
        begin = begin + lengths[d]

    def wide(parts, t):
        per = TILE // LANES
        return jnp.concatenate([parts[(t * per + k) % chunks] for k in range(per)], axis=1)

    def query_tile(g, t):
        at, left, parts = t * TILE, TILE, []
        while left:
            r, row = divmod(at, tok)
            n = min(left, tok - row)
            h = g * group + r
            parts.append(q_ref[row : row + n, h * HEAD_DIM : (h + 1) * HEAD_DIM])
            at, left = at + n, left - n
        return parts[0] if len(parts) == 1 else jnp.concatenate(parts, axis=0)

    def fold(kv_ref, mode, source):
        fresh = mode == "own"
        total_tiles = heads * tiles
        tops, shifts, fades = {}, {}, {}

        def score_stage(n):
            g, t = divmod(n, tiles)
            key = kv_ref[0, :, g * HEAD_DIM : (g + 1) * HEAD_DIM]
            score = lax.dot_general(
                key, query_tile(g, t), (((1,), (1,)), ((), ())), preferred_element_type=jnp.float32
            )
            if mode == "own":
                score = score + wide([mask_ref[:, k * LANES : (k + 1) * LANES] for k in range(chunks)], t)
            elif mode == "part":
                score = score + wide([mask_ref[:, :LANES]] * chunks, t)
            s_ref[n % DEPTH] = score
            top = jnp.max(score, axis=0, keepdims=True)
            shifts[n] = top
            if not fresh:
                joins = wide(low, t) == lead
                old = source[n, HEAD_DIM : HEAD_DIM + 1, :]
                top = jnp.where(joins, jnp.maximum(top, old), old)
                shifts[n] = jnp.where(joins, top, -NEG)
                fades[n] = jnp.exp2((old - top) * SCALE)
            tops[n] = top

        def weight_stage(n):
            weight = jnp.exp2((s_ref[n % DEPTH] - shifts[n]) * SCALE)
            p_ref[n % DEPTH] = weight.astype(jnp.bfloat16)
            total = jnp.sum(weight, axis=0, keepdims=True)
            if not fresh:
                total = total + source[n, HEAD_DIM + 1 : HEAD_DIM + 2, :] * fades[n]
            state[n, HEAD_DIM : HEAD_DIM + 1, :] = tops[n]
            state[n, HEAD_DIM + 1 : HEAD_DIM + 2, :] = total

        def value_stage(n):
            g, _ = divmod(n, tiles)
            value = kv_ref[1, :, g * HEAD_DIM : (g + 1) * HEAD_DIM]
            acc = lax.dot_general(
                value, p_ref[n % DEPTH], (((0,), (0,)), ((), ())), preferred_element_type=jnp.float32
            )
            if not fresh:
                acc = acc + source[n, :HEAD_DIM, :] * fades[n]
            state[n, :HEAD_DIM, :] = acc

        for i in range(0, total_tiles + 2 * BATCH, BATCH):
            for k in range(BATCH):
                n = i + k
                if n < total_tiles:
                    score_stage(n)
                if 0 <= n - BATCH < total_tiles:
                    weight_stage(n - BATCH)
                if 0 <= n - 2 * BATCH < total_tiles:
                    value_stage(n - 2 * BATCH)

    if not first and final:
        state[...] = state_in[...]
    for j, (kv_ref, (even_back, odd_back)) in enumerate(zip(kv_refs, blocks)):
        if first and j == 0:
            key_row = anchor + lax.broadcasted_iota(jnp.int32, (tok, LANES), 0)
            for k in range(chunks):
                live = (key_row >= low[k]) & (key_row <= pos[k])
                mask_ref[:, k * LANES : (k + 1) * LANES] = jnp.where(live, 0.0, NEG)
            fold(kv_ref, "own", None)
            continue
        start = anchor - jnp.where(odd, odd_back, even_back) * tok

        @pl.when((start >= 0) & (lead < start + tok))
        def _():
            key_row = start + lax.broadcasted_iota(jnp.int32, (tok, LANES), 0)
            mask_ref[:, :LANES] = jnp.where(key_row >= lead, 0.0, NEG)
            fold(kv_ref, "part", state)

    if final:
        for g in range(heads):
            for t in range(tiles):
                n = g * tiles + t
                share = 1.0 / state[n, HEAD_DIM + 1 : HEAD_DIM + 2, :]
                done = (state[n, :HEAD_DIM, :] * share).T.astype(jnp.bfloat16)
                at, left = t * TILE, TILE
                while left:
                    r, row = divmod(at, tok)
                    m = min(left, tok - row)
                    h = g * group + r
                    o = at - t * TILE
                    out_ref[row : row + m, h * HEAD_DIM : (h + 1) * HEAD_DIM] = done[o : o + m, :]
                    at, left = at + m, left - m


def attend(lengths, queries, kvs, blocks, state, final):
    tok, width = queries.shape
    heads = kvs[0].shape[-1] // HEAD_DIM
    group = width // kvs[0].shape[-1]
    count = heads * group * tok // TILE
    first = state is None
    state_shape = jax.ShapeDtypeStruct((count, HEAD_DIM + 8, TILE), jnp.float32)
    vmem = pl.BlockSpec(memory_space=pltpu.VMEM)
    args = [lengths, queries, *kvs] + ([] if first else [state])
    aliases = {} if first or final else {len(args) - 1: 0}
    flops = 4 * tok * tok * width * len(blocks)
    return pl.pallas_call(
        functools.partial(attend_kernel, blocks, first, final, tok, heads, group),
        out_shape=jax.ShapeDtypeStruct((tok, width), jnp.bfloat16) if final else state_shape,
        in_specs=[pl.BlockSpec(memory_space=pltpu.SMEM)] + [vmem] * (len(args) - 1),
        out_specs=vmem,
        scratch_shapes=[
            pltpu.VMEM((DEPTH, tok, TILE), jnp.float32),
            pltpu.VMEM((DEPTH, tok, TILE), jnp.bfloat16),
            pltpu.VMEM((tok, tok), jnp.float32),
            *([pltpu.VMEM(state_shape.shape, jnp.float32)] if final else []),
        ],
        input_output_aliases=aliases,
        compiler_params=pltpu.CompilerParams(vmem_limit_bytes=16 << 20),
        cost_estimate=pl.CostEstimate(flops=flops, bytes_accessed=1 << 20, transcendentals=0),
    )(*args)


def body(queries, keys, values, lengths):
    ways = routes(lax.axis_size("cp"))

    def move(x, way):
        return lax.ppermute(x, "cp", ways[way])

    after = lax.optimization_barrier
    own = jnp.stack([keys, values])
    step = functools.partial(attend, lengths, queries)
    got1 = move(own, "cross")
    mix1 = move(own, "back1")
    state = step([own], [(0, 0)], None, False)
    state, got1 = after((state, got1))
    got2 = move(got1, "ahead")
    mate1 = move(got1, "swap")
    far2 = move(mix1, "back2")
    state = step([mix1, got1], [(NONE, 1), (1, 3)], state, False)
    state, mate1 = after((state, mate1))
    state = step([mate1], [(2, 2)], state, False)
    state, got2 = after((state, got2))
    got3 = move(got2, "ahead")
    mate2 = move(got2, "swap")
    state = step([got2], [(3, 5)], state, False)
    state, mate2 = after((state, mate2))
    state, far2 = after((state, far2))
    state = step([mate2, far2], [(4, 4), (7, NONE)], state, False)
    state, got3 = after((state, got3))
    mate3 = move(got3, "swap")
    state = step([got3], [(5, 7)], state, False)
    state, mate3 = after((state, mate3))
    return step([mate3], [(6, 6)], state, True)


def solution(mesh):
    in_specs = (P("cp", "tp"), P("cp", "tp"), P("cp", "tp"), P())
    out_specs = P("cp", "tp")
    return jax.shard_map(body, mesh=mesh, in_specs=in_specs, out_specs=out_specs, check_vma=False)
```

```python
import functools

import jax
import jax.numpy as jnp
from jax import lax
from jax.experimental import pallas as pl
from jax.experimental.pallas import tpu as pltpu
from jax.sharding import PartitionSpec as P


HEAD_DIM = 128
RING = 8
TILE = 256
LANES = 128
NEG = -1e30
SCALE = HEAD_DIM**-0.5 * 1.4426950408889634
NONE = 1 << 20
DEPTH = 6
BATCH = 3


def routes(count):
    chips = count // 2
    dev = lambda n, c: 2 * n + c
    back = lambda n: n - n % RING + (n % RING - RING // 4) % RING
    inside = [n for n in range(chips) if n + 4 < chips]
    return {
        "cross": [(dev(n, c), dev(n + 1, 1 - c)) for n in range(chips - 1) for c in (0, 1)],
        "ahead": [(dev(n, c), dev(n + 1, c)) for n in range(chips - 1) for c in (0, 1)],
        "swap": [(dev(n, c), dev(n, 1 - c)) for n in range(chips) for c in (0, 1)],
        "back1": [(dev(n, 1), dev(back(n), 0)) for n in inside] + [(dev(n, 0), dev(n, 1)) for n in range(chips)],
        "back2": [(dev(back(n), 0), dev(n + 4, 0)) for n in inside],
    }


def attend_kernel(blocks, first, final, tok, heads, group, *refs):
    refs = list(refs)
    lengths, q_ref = refs.pop(0), refs.pop(0)
    kv_refs = []
    while len(kv_refs) < len(blocks):
        ref = refs.pop(0)
        kv_refs += [ref] if len(ref.shape) == 3 else [ref.at[j] for j in range(ref.shape[0])]
    state_in = None if first else refs.pop(0)
    out_ref = refs.pop(0)
    s_ref, p_ref, mask_ref = refs.pop(0), refs.pop(0), refs.pop(0)
    state = refs.pop(0) if final else out_ref
    me = lax.axis_index("cp")
    anchor = me * tok
    odd = me % 2 == 1
    rows = group * tok
    tiles = rows // TILE
    chunks = tok // LANES

    lane = lax.broadcasted_iota(jnp.int32, (1, LANES), 1)
    pos = [anchor + k * LANES + lane for k in range(chunks)]
    low = [jnp.zeros((1, LANES), jnp.int32) for _ in range(chunks)]
    begin = jnp.int32(0)
    lead = jnp.int32(0)
    for d in range(lengths.shape[0]):
        low = [jnp.where(p >= begin, begin, l) for p, l in zip(pos, low)]
        lead = jnp.where(begin <= anchor, begin, lead)
        begin = begin + lengths[d]

    def wide(parts, t):
        per = TILE // LANES
        return jnp.concatenate([parts[(t * per + k) % chunks] for k in range(per)], axis=1)

    def query_tile(g, t):
        at, left, parts = t * TILE, TILE, []
        while left:
            r, row = divmod(at, tok)
            n = min(left, tok - row)
            h = g * group + r
            parts.append(q_ref[row : row + n, h * HEAD_DIM : (h + 1) * HEAD_DIM])
            at, left = at + n, left - n
        return parts[0] if len(parts) == 1 else jnp.concatenate(parts, axis=0)

    def fold(kv_ref, mode, source):
        fresh = mode == "own"
        total_tiles = heads * tiles
        tops, shifts, fades = {}, {}, {}

        def score_stage(n):
            g, t = divmod(n, tiles)
            key = kv_ref[0, :, g * HEAD_DIM : (g + 1) * HEAD_DIM]
            score = lax.dot_general(
                key, query_tile(g, t), (((1,), (1,)), ((), ())), preferred_element_type=jnp.float32
            )
            if mode == "own":
                score = score + wide([mask_ref[:, k * LANES : (k + 1) * LANES] for k in range(chunks)], t)
            elif mode == "part":
                score = score + wide([mask_ref[:, :LANES]] * chunks, t)
            s_ref[n % DEPTH] = score
            top = jnp.max(score, axis=0, keepdims=True)
            shifts[n] = top
            if not fresh:
                joins = wide(low, t) == lead
                old = source[n, HEAD_DIM : HEAD_DIM + 1, :]
                top = jnp.where(joins, jnp.maximum(top, old), old)
                shifts[n] = jnp.where(joins, top, -NEG)
                fades[n] = jnp.exp2((old - top) * SCALE)
            tops[n] = top

        def weight_stage(n):
            weight = jnp.exp2((s_ref[n % DEPTH] - shifts[n]) * SCALE)
            p_ref[n % DEPTH] = weight.astype(jnp.bfloat16)
            total = jnp.sum(weight, axis=0, keepdims=True)
            if not fresh:
                total = total + source[n, HEAD_DIM + 1 : HEAD_DIM + 2, :] * fades[n]
            state[n, HEAD_DIM : HEAD_DIM + 1, :] = tops[n]
            state[n, HEAD_DIM + 1 : HEAD_DIM + 2, :] = total

        def value_stage(n):
            g, _ = divmod(n, tiles)
            value = kv_ref[1, :, g * HEAD_DIM : (g + 1) * HEAD_DIM]
            acc = lax.dot_general(
                value, p_ref[n % DEPTH], (((0,), (0,)), ((), ())), preferred_element_type=jnp.float32
            )
            if not fresh:
                acc = acc + source[n, :HEAD_DIM, :] * fades[n]
            state[n, :HEAD_DIM, :] = acc

        for i in range(0, total_tiles + 2 * BATCH, BATCH):
            for k in range(BATCH):
                n = i + k
                if n < total_tiles:
                    score_stage(n)
                if 0 <= n - BATCH < total_tiles:
                    weight_stage(n - BATCH)
                if 0 <= n - 2 * BATCH < total_tiles:
                    value_stage(n - 2 * BATCH)

    if not first and final:
        state[...] = state_in[...]
    for j, (kv_ref, (even_back, odd_back)) in enumerate(zip(kv_refs, blocks)):
        if first and j == 0:
            key_row = anchor + lax.broadcasted_iota(jnp.int32, (tok, LANES), 0)
            for k in range(chunks):
                live = (key_row >= low[k]) & (key_row <= pos[k])
                mask_ref[:, k * LANES : (k + 1) * LANES] = jnp.where(live, 0.0, NEG)
            fold(kv_ref, "own", None)
            continue
        start = anchor - jnp.where(odd, odd_back, even_back) * tok

        @pl.when((start >= 0) & (lead < start + tok))
        def _():
            key_row = start + lax.broadcasted_iota(jnp.int32, (tok, LANES), 0)
            mask_ref[:, :LANES] = jnp.where(key_row >= lead, 0.0, NEG)
            fold(kv_ref, "part", state)

    if final:
        for g in range(heads):
            for t in range(tiles):
                n = g * tiles + t
                share = 1.0 / state[n, HEAD_DIM + 1 : HEAD_DIM + 2, :]
                done = (state[n, :HEAD_DIM, :] * share).T.astype(jnp.bfloat16)
                at, left = t * TILE, TILE
                while left:
                    r, row = divmod(at, tok)
                    m = min(left, tok - row)
                    h = g * group + r
                    o = at - t * TILE
                    out_ref[row : row + m, h * HEAD_DIM : (h + 1) * HEAD_DIM] = done[o : o + m, :]
                    at, left = at + m, left - m


def attend(lengths, queries, kvs, blocks, state, final):
    tok, width = queries.shape
    heads = kvs[0].shape[-1] // HEAD_DIM
    group = width // kvs[0].shape[-1]
    count = heads * group * tok // TILE
    first = state is None
    state_shape = jax.ShapeDtypeStruct((count, HEAD_DIM + 8, TILE), jnp.float32)
    vmem = pl.BlockSpec(memory_space=pltpu.VMEM)
    args = [lengths, queries, *kvs] + ([] if first else [state])
    aliases = {} if first or final else {len(args) - 1: 0}
    flops = 4 * tok * tok * width * len(blocks)
    return pl.pallas_call(
        functools.partial(attend_kernel, blocks, first, final, tok, heads, group),
        out_shape=jax.ShapeDtypeStruct((tok, width), jnp.bfloat16) if final else state_shape,
        in_specs=[pl.BlockSpec(memory_space=pltpu.SMEM)] + [vmem] * (len(args) - 1),
        out_specs=vmem,
        scratch_shapes=[
            pltpu.VMEM((DEPTH, tok, TILE), jnp.float32),
            pltpu.VMEM((DEPTH, tok, TILE), jnp.bfloat16),
            pltpu.VMEM((tok, tok), jnp.float32),
            *([pltpu.VMEM(state_shape.shape, jnp.float32)] if final else []),
        ],
        input_output_aliases=aliases,
        compiler_params=pltpu.CompilerParams(vmem_limit_bytes=16 << 20),
        cost_estimate=pl.CostEstimate(flops=flops, bytes_accessed=1 << 20, transcendentals=0),
    )(*args)


def body(queries, keys, values, lengths):
    ways = routes(lax.axis_size("cp"))

    def move(x, way):
        return lax.ppermute(x, "cp", ways[way])

    after = lax.optimization_barrier
    own = jnp.stack([keys, values])
    step = functools.partial(attend, lengths, queries)
    got1 = move(own, "cross")
    mix1 = move(own, "back1")
    state = step([own], [(0, 0)], None, False)
    state, got1 = after((state, got1))
    got2 = move(got1, "ahead")
    mate1 = move(got1, "swap")
    far2 = move(mix1, "back2")
    state = step([mix1, got1], [(NONE, 1), (1, 3)], state, False)
    state, mate1 = after((state, mate1))
    state = step([mate1], [(2, 2)], state, False)
    state, got2 = after((state, got2))
    got3 = move(got2, "ahead")
    mate2 = move(got2, "swap")
    state = step([got2], [(3, 5)], state, False)
    state, mate2 = after((state, mate2))
    state, far2 = after((state, far2))
    state = step([mate2, far2], [(4, 4), (7, NONE)], state, False)
    state, got3 = after((state, got3))
    mate3 = move(got3, "swap")
    state = step([got3], [(5, 7)], state, False)
    state, mate3 = after((state, mate3))
    return step([mate3], [(6, 6)], state, True)


def solution(mesh):
    in_specs = (P("cp", "tp"), P("cp", "tp"), P("cp", "tp"), P())
    out_specs = P("cp", "tp")
    return jax.shard_map(body, mesh=mesh, in_specs=in_specs, out_specs=out_specs, check_vma=False)
```

```python
import functools

import jax
import jax.numpy as jnp
from jax import lax
from jax.experimental import pallas as pl
from jax.experimental.pallas import tpu as pltpu
from jax.sharding import PartitionSpec as P


HEAD_DIM = 128
RING = 8
TILE = 256
LANES = 128
NEG = -1e30
SCALE = HEAD_DIM**-0.5 * 1.4426950408889634
NONE = 1 << 20
DEPTH = 6
BATCH = 3


def routes(count):
    chips = count // 2
    dev = lambda n, c: 2 * n + c
    back = lambda n: n - n % RING + (n % RING - RING // 4) % RING
    inside = [n for n in range(chips) if n + 4 < chips]
    return {
        "ahead": [(dev(n, c), dev(n + 1, c)) for n in range(chips - 1) for c in (0, 1)],
        "swap": [(dev(n, c), dev(n, 1 - c)) for n in range(chips) for c in (0, 1)],
        "back1": [(dev(n, 1), dev(back(n), 0)) for n in inside] + [(dev(n, 0), dev(n, 1)) for n in range(chips)],
        "back2": [(dev(back(n), 0), dev(n + 4, 0)) for n in inside],
    }


def attend_kernel(blocks, first, final, tok, heads, group, *refs):
    refs = list(refs)
    lengths, q_ref = refs.pop(0), refs.pop(0)
    kv_refs = []
    while len(kv_refs) < len(blocks):
        ref = refs.pop(0)
        kv_refs += [ref] if len(ref.shape) == 3 else [ref.at[j] for j in range(ref.shape[0])]
    state_in = None if first else refs.pop(0)
    out_ref = refs.pop(0)
    s_ref, p_ref, mask_ref = refs.pop(0), refs.pop(0), refs.pop(0)
    state = refs.pop(0) if final else out_ref
    me = lax.axis_index("cp")
    anchor = me * tok
    odd = me % 2 == 1
    rows = group * tok
    tiles = rows // TILE
    chunks = tok // LANES

    lane = lax.broadcasted_iota(jnp.int32, (1, LANES), 1)
    pos = [anchor + k * LANES + lane for k in range(chunks)]
    low = [jnp.zeros((1, LANES), jnp.int32) for _ in range(chunks)]
    begin = jnp.int32(0)
    lead = jnp.int32(0)
    for d in range(lengths.shape[0]):
        low = [jnp.where(p >= begin, begin, l) for p, l in zip(pos, low)]
        lead = jnp.where(begin <= anchor, begin, lead)
        begin = begin + lengths[d]

    def wide(parts, t):
        per = TILE // LANES
        return jnp.concatenate([parts[(t * per + k) % chunks] for k in range(per)], axis=1)

    def query_tile(g, t):
        at, left, parts = t * TILE, TILE, []
        while left:
            r, row = divmod(at, tok)
            n = min(left, tok - row)
            h = g * group + r
            parts.append(q_ref[row : row + n, h * HEAD_DIM : (h + 1) * HEAD_DIM])
            at, left = at + n, left - n
        return parts[0] if len(parts) == 1 else jnp.concatenate(parts, axis=0)

    def fold(kv_ref, mode, source):
        fresh = mode == "own"
        total_tiles = heads * tiles
        tops, shifts, fades = {}, {}, {}

        def score_stage(n):
            g, t = divmod(n, tiles)
            key = kv_ref[0, :, g * HEAD_DIM : (g + 1) * HEAD_DIM]
            score = lax.dot_general(
                key, query_tile(g, t), (((1,), (1,)), ((), ())), preferred_element_type=jnp.float32
            )
            if mode == "own":
                score = score + wide([mask_ref[:, k * LANES : (k + 1) * LANES] for k in range(chunks)], t)
            elif mode == "part":
                score = score + wide([mask_ref[:, :LANES]] * chunks, t)
            s_ref[n % DEPTH] = score
            top = jnp.max(score, axis=0, keepdims=True)
            shifts[n] = top
            if not fresh:
                joins = wide(low, t) == lead
                old = source[n, HEAD_DIM : HEAD_DIM + 1, :]
                top = jnp.where(joins, jnp.maximum(top, old), old)
                shifts[n] = jnp.where(joins, top, -NEG)
                fades[n] = jnp.exp2((old - top) * SCALE)
            tops[n] = top

        def weight_stage(n):
            weight = jnp.exp2((s_ref[n % DEPTH] - shifts[n]) * SCALE)
            p_ref[n % DEPTH] = weight.astype(jnp.bfloat16)
            total = jnp.sum(weight, axis=0, keepdims=True)
            if not fresh:
                total = total + source[n, HEAD_DIM + 1 : HEAD_DIM + 2, :] * fades[n]
            state[n, HEAD_DIM : HEAD_DIM + 1, :] = tops[n]
            state[n, HEAD_DIM + 1 : HEAD_DIM + 2, :] = total

        def value_stage(n):
            g, _ = divmod(n, tiles)
            value = kv_ref[1, :, g * HEAD_DIM : (g + 1) * HEAD_DIM]
            acc = lax.dot_general(
                value, p_ref[n % DEPTH], (((0,), (0,)), ((), ())), preferred_element_type=jnp.float32
            )
            if not fresh:
                acc = acc + source[n, :HEAD_DIM, :] * fades[n]
            state[n, :HEAD_DIM, :] = acc

        for i in range(0, total_tiles + 2 * BATCH, BATCH):
            for k in range(BATCH):
                n = i + k
                if n < total_tiles:
                    score_stage(n)
                if 0 <= n - BATCH < total_tiles:
                    weight_stage(n - BATCH)
                if 0 <= n - 2 * BATCH < total_tiles:
                    value_stage(n - 2 * BATCH)

    if not first and final:
        state[...] = state_in[...]
    for j, (kv_ref, (even_back, odd_back)) in enumerate(zip(kv_refs, blocks)):
        if first and j == 0:
            key_row = anchor + lax.broadcasted_iota(jnp.int32, (tok, LANES), 0)
            for k in range(chunks):
                live = (key_row >= low[k]) & (key_row <= pos[k])
                mask_ref[:, k * LANES : (k + 1) * LANES] = jnp.where(live, 0.0, NEG)
            fold(kv_ref, "own", None)
            continue
        start = anchor - jnp.where(odd, odd_back, even_back) * tok

        @pl.when((start >= 0) & (lead < start + tok))
        def _():
            key_row = start + lax.broadcasted_iota(jnp.int32, (tok, LANES), 0)
            mask_ref[:, :LANES] = jnp.where(key_row >= lead, 0.0, NEG)
            fold(kv_ref, "part", state)

    if final:
        for g in range(heads):
            for t in range(tiles):
                n = g * tiles + t
                share = 1.0 / state[n, HEAD_DIM + 1 : HEAD_DIM + 2, :]
                done = (state[n, :HEAD_DIM, :] * share).T.astype(jnp.bfloat16)
                at, left = t * TILE, TILE
                while left:
                    r, row = divmod(at, tok)
                    m = min(left, tok - row)
                    h = g * group + r
                    o = at - t * TILE
                    out_ref[row : row + m, h * HEAD_DIM : (h + 1) * HEAD_DIM] = done[o : o + m, :]
                    at, left = at + m, left - m


def attend(lengths, queries, kvs, blocks, state, final):
    tok, width = queries.shape
    heads = kvs[0].shape[-1] // HEAD_DIM
    group = width // kvs[0].shape[-1]
    count = heads * group * tok // TILE
    first = state is None
    state_shape = jax.ShapeDtypeStruct((count, HEAD_DIM + 8, TILE), jnp.float32)
    vmem = pl.BlockSpec(memory_space=pltpu.VMEM)
    args = [lengths, queries, *kvs] + ([] if first else [state])
    aliases = {} if first or final else {len(args) - 1: 0}
    flops = 4 * tok * tok * width * len(blocks)
    return pl.pallas_call(
        functools.partial(attend_kernel, blocks, first, final, tok, heads, group),
        out_shape=jax.ShapeDtypeStruct((tok, width), jnp.bfloat16) if final else state_shape,
        in_specs=[pl.BlockSpec(memory_space=pltpu.SMEM)] + [vmem] * (len(args) - 1),
        out_specs=vmem,
        scratch_shapes=[
            pltpu.VMEM((DEPTH, tok, TILE), jnp.float32),
            pltpu.VMEM((DEPTH, tok, TILE), jnp.bfloat16),
            pltpu.VMEM((tok, tok), jnp.float32),
            *([pltpu.VMEM(state_shape.shape, jnp.float32)] if final else []),
        ],
        input_output_aliases=aliases,
        compiler_params=pltpu.CompilerParams(vmem_limit_bytes=16 << 20),
        cost_estimate=pl.CostEstimate(flops=flops, bytes_accessed=1 << 20, transcendentals=0),
    )(*args)


def body(queries, keys, values, lengths):
    ways = routes(lax.axis_size("cp"))

    def move(x, way):
        return lax.ppermute(x, "cp", ways[way])

    after = lax.optimization_barrier
    own = jnp.stack([keys, values])
    step = functools.partial(attend, lengths, queries)
    got1 = move(own, "ahead")
    mix1 = move(own, "back1")
    state = step([own], [(0, 0)], None, False)
    state, got1 = after((state, got1))
    got2 = move(got1, "ahead")
    mate1 = move(got1, "swap")
    far2 = move(mix1, "back2")
    state = step([mix1, got1], [(NONE, 1), (2, 2)], state, False)
    state, mate1 = after((state, mate1))
    state = step([mate1], [(1, 3)], state, False)
    state, got2 = after((state, got2))
    got3 = move(got2, "ahead")
    mate2 = move(got2, "swap")
    state = step([got2], [(4, 4)], state, False)
    state, mate2 = after((state, mate2))
    state, far2 = after((state, far2))
    state = step([mate2, far2], [(3, 5), (7, NONE)], state, False)
    state, got3 = after((state, got3))
    mate3 = move(got3, "swap")
    state = step([got3], [(6, 6)], state, False)
    state, mate3 = after((state, mate3))
    return step([mate3], [(5, 7)], state, True)


def solution(mesh):
    in_specs = (P("cp", "tp"), P("cp", "tp"), P("cp", "tp"), P())
    out_specs = P("cp", "tp")
    return jax.shard_map(body, mesh=mesh, in_specs=in_specs, out_specs=out_specs, check_vma=False)
```

```python
import functools

import jax
import jax.numpy as jnp
from jax import lax
from jax.experimental import pallas as pl
from jax.experimental.pallas import tpu as pltpu
from jax.sharding import PartitionSpec as P


HEAD_DIM = 128
RING = 8
TILE = 256
LANES = 128
NEG = -1e30
SCALE = HEAD_DIM**-0.5 * 1.4426950408889634
NONE = 1 << 20
DEPTH = 6
BATCH = 3


def routes(count):
    chips = count // 2
    dev = lambda n, c: 2 * n + c
    back = lambda n: n - n % RING + (n % RING - RING // 4) % RING
    inside = [n for n in range(chips) if n + 4 < chips]
    return {
        "ahead": [(dev(n, c), dev(n + 1, c)) for n in range(chips - 1) for c in (0, 1)],
        "swap": [(dev(n, c), dev(n, 1 - c)) for n in range(chips) for c in (0, 1)],
        "back1": [(dev(n, 1), dev(back(n), 0)) for n in inside] + [(dev(n, 0), dev(n, 1)) for n in range(chips)],
        "back2": [(dev(back(n), 0), dev(n + 4, 0)) for n in inside],
    }


def attend_kernel(blocks, first, final, tok, heads, group, *refs):
    refs = list(refs)
    lengths, q_ref = refs.pop(0), refs.pop(0)
    kv_refs = []
    while len(kv_refs) < len(blocks):
        ref = refs.pop(0)
        kv_refs += [ref] if len(ref.shape) == 3 else [ref.at[j] for j in range(ref.shape[0])]
    if not first:
        refs.pop(0)
    out_ref = refs.pop(0)
    state = refs.pop(0) if final else out_ref
    s_ref, p_ref, mask_ref = refs.pop(0), refs.pop(0), refs.pop(0)
    me = lax.axis_index("cp")
    anchor = me * tok
    odd = me % 2 == 1
    rows = group * tok
    tiles = rows // TILE
    chunks = tok // LANES

    lane = lax.broadcasted_iota(jnp.int32, (1, LANES), 1)
    pos = [anchor + k * LANES + lane for k in range(chunks)]
    low = [jnp.zeros((1, LANES), jnp.int32) for _ in range(chunks)]
    begin = jnp.int32(0)
    lead = jnp.int32(0)
    for d in range(lengths.shape[0]):
        low = [jnp.where(p >= begin, begin, l) for p, l in zip(pos, low)]
        lead = jnp.where(begin <= anchor, begin, lead)
        begin = begin + lengths[d]

    def wide(parts, t):
        per = TILE // LANES
        return jnp.concatenate([parts[(t * per + k) % chunks] for k in range(per)], axis=1)

    def query_tile(g, t):
        at, left, parts = t * TILE, TILE, []
        while left:
            r, row = divmod(at, tok)
            n = min(left, tok - row)
            h = g * group + r
            parts.append(q_ref[row : row + n, h * HEAD_DIM : (h + 1) * HEAD_DIM])
            at, left = at + n, left - n
        return parts[0] if len(parts) == 1 else jnp.concatenate(parts, axis=0)

    def fold(kv_ref, mode, source):
        fresh = mode == "own"
        total_tiles = heads * tiles
        tops, shifts, fades = {}, {}, {}

        def score_stage(n):
            g, t = divmod(n, tiles)
            key = kv_ref[0, :, g * HEAD_DIM : (g + 1) * HEAD_DIM]
            score = lax.dot_general(
                key, query_tile(g, t), (((1,), (1,)), ((), ())), preferred_element_type=jnp.float32
            )
            if mode == "own":
                score = score + wide([mask_ref[:, k * LANES : (k + 1) * LANES] for k in range(chunks)], t)
            elif mode == "part":
                score = score + wide([mask_ref[:, :LANES]] * chunks, t)
            s_ref[n % DEPTH] = score
            top = jnp.max(score, axis=0, keepdims=True)
            shifts[n] = top
            if not fresh:
                joins = wide(low, t) == lead
                old = source[n, HEAD_DIM : HEAD_DIM + 1, :]
                top = jnp.where(joins, jnp.maximum(top, old), old)
                shifts[n] = jnp.where(joins, top, -NEG)
                fades[n] = jnp.exp2((old - top) * SCALE)
            tops[n] = top

        def weight_stage(n):
            weight = jnp.exp2((s_ref[n % DEPTH] - shifts[n]) * SCALE)
            p_ref[n % DEPTH] = weight.astype(jnp.bfloat16)
            total = jnp.sum(weight, axis=0, keepdims=True)
            if not fresh:
                total = total + source[n, HEAD_DIM + 1 : HEAD_DIM + 2, :] * fades[n]
            state[n, HEAD_DIM : HEAD_DIM + 1, :] = tops[n]
            state[n, HEAD_DIM + 1 : HEAD_DIM + 2, :] = total

        def value_stage(n):
            g, _ = divmod(n, tiles)
            value = kv_ref[1, :, g * HEAD_DIM : (g + 1) * HEAD_DIM]
            acc = lax.dot_general(
                value, p_ref[n % DEPTH], (((0,), (0,)), ((), ())), preferred_element_type=jnp.float32
            )
            if not fresh:
                acc = acc + source[n, :HEAD_DIM, :] * fades[n]
            state[n, :HEAD_DIM, :] = acc

        for i in range(0, total_tiles + 2 * BATCH, BATCH):
            for k in range(BATCH):
                n = i + k
                if n < total_tiles:
                    score_stage(n)
                if 0 <= n - BATCH < total_tiles:
                    weight_stage(n - BATCH)
                if 0 <= n - 2 * BATCH < total_tiles:
                    value_stage(n - 2 * BATCH)

    for j, (kv_ref, (even_back, odd_back)) in enumerate(zip(kv_refs, blocks)):
        if first and j == 0:
            key_row = anchor + lax.broadcasted_iota(jnp.int32, (tok, LANES), 0)
            for k in range(chunks):
                live = (key_row >= low[k]) & (key_row <= pos[k])
                mask_ref[:, k * LANES : (k + 1) * LANES] = jnp.where(live, 0.0, NEG)
            fold(kv_ref, "own", None)
            continue
        start = anchor - jnp.where(odd, odd_back, even_back) * tok

        @pl.when((start >= 0) & (lead < start + tok))
        def _():
            key_row = start + lax.broadcasted_iota(jnp.int32, (tok, LANES), 0)
            mask_ref[:, :LANES] = jnp.where(key_row >= lead, 0.0, NEG)
            fold(kv_ref, "part", state)

    if final:
        for g in range(heads):
            for t in range(tiles):
                n = g * tiles + t
                share = 1.0 / state[n, HEAD_DIM + 1 : HEAD_DIM + 2, :]
                done = (state[n, :HEAD_DIM, :] * share).T.astype(jnp.bfloat16)
                at, left = t * TILE, TILE
                while left:
                    r, row = divmod(at, tok)
                    m = min(left, tok - row)
                    h = g * group + r
                    o = at - t * TILE
                    out_ref[row : row + m, h * HEAD_DIM : (h + 1) * HEAD_DIM] = done[o : o + m, :]
                    at, left = at + m, left - m


def attend(lengths, queries, kvs, blocks, state, final):
    tok, width = queries.shape
    heads = kvs[0].shape[-1] // HEAD_DIM
    group = width // kvs[0].shape[-1]
    count = heads * group * tok // TILE
    first = state is None
    state_shape = jax.ShapeDtypeStruct((count, HEAD_DIM + 8, TILE), jnp.float32)
    vmem = pl.BlockSpec(memory_space=pltpu.VMEM)
    args = [lengths, queries, *kvs] + ([] if first else [state])
    aliases = {} if first else {len(args) - 1: int(final)}
    attended = jax.ShapeDtypeStruct((tok, width), jnp.bfloat16)
    flops = 4 * tok * tok * width * len(blocks)
    return pl.pallas_call(
        functools.partial(attend_kernel, blocks, first, final, tok, heads, group),
        out_shape=(attended, state_shape) if final else state_shape,
        in_specs=[pl.BlockSpec(memory_space=pltpu.SMEM)] + [vmem] * (len(args) - 1),
        out_specs=(vmem, vmem) if final else vmem,
        scratch_shapes=[
            pltpu.VMEM((DEPTH, tok, TILE), jnp.float32),
            pltpu.VMEM((DEPTH, tok, TILE), jnp.bfloat16),
            pltpu.VMEM((tok, tok), jnp.float32),
        ],
        input_output_aliases=aliases,
        compiler_params=pltpu.CompilerParams(vmem_limit_bytes=16 << 20),
        cost_estimate=pl.CostEstimate(flops=flops, bytes_accessed=1 << 20, transcendentals=0),
    )(*args)


def body(queries, keys, values, lengths):
    ways = routes(lax.axis_size("cp"))

    def move(x, way):
        return lax.ppermute(x, "cp", ways[way])

    after = lax.optimization_barrier
    own = jnp.stack([keys, values])
    step = functools.partial(attend, lengths, queries)
    got1 = move(own, "ahead")
    mix1 = move(own, "back1")
    state = step([own], [(0, 0)], None, False)
    state, got1 = after((state, got1))
    got2 = move(got1, "ahead")
    mate1 = move(got1, "swap")
    far2 = move(mix1, "back2")
    state = step([mix1, got1], [(NONE, 1), (2, 2)], state, False)
    state, mate1 = after((state, mate1))
    state = step([mate1], [(1, 3)], state, False)
    state, got2 = after((state, got2))
    got3 = move(got2, "ahead")
    mate2 = move(got2, "swap")
    state = step([got2], [(4, 4)], state, False)
    state, mate2 = after((state, mate2))
    state, far2 = after((state, far2))
    state = step([mate2, far2], [(3, 5), (7, NONE)], state, False)
    state, got3 = after((state, got3))
    mate3 = move(got3, "swap")
    state = step([got3], [(6, 6)], state, False)
    state, mate3 = after((state, mate3))
    return step([mate3], [(5, 7)], state, True)[0]


def solution(mesh):
    in_specs = (P("cp", "tp"), P("cp", "tp"), P("cp", "tp"), P())
    out_specs = P("cp", "tp")
    return jax.shard_map(body, mesh=mesh, in_specs=in_specs, out_specs=out_specs, check_vma=False)
```
